32 devices in a mesh: seq: 8 (over z, y), mp: 4 (over x, core).
Axes of the slice: x: 2, y: 2, z: 4, core: 2. Of those that a mesh axis runs over, the one named last changes fastest.
Arguments:
- ssm_input: bfloat16 [8192, 5120], P('seq', 'mp'), may hold values from -6 to 6
- gate_input: bfloat16 [8192, 5120], P('seq', 'mp'), may hold values from -6 to 6
- state_in: bfloat16 [8192, 128], P('seq'), may hold values from -6 to 6
- state_out: bfloat16 [8192, 128], P('seq'), may hold values from -0.5 to 0.5
- step_size: float32 [8192, 80], P('seq', 'mp'), may hold values from 0.05 to 0.2
- log_decay: float32 [8192, 80], P('seq', 'mp'), may hold values from -2 to 0
- skip_gain: float32 [80], P('mp'), may hold values from 0.5 to 2
- norm_gain: bfloat16 [5120], P('mp'), may hold values from 0.099609375 to 1.8984375
- out_weight: bfloat16 [5120, 2560], P('mp'), may hold values from -0.078125 to 0.078125
Outputs:
- layer_out: bfloat16 [8192, 2560], P(('seq', 'mp'))
The draws below stay inside these ranges and needn't reach their ends.
All inputs are finite; a program needn't handle non-finite values.
Results may differ from the reference program's by a relative error of at most 0.011.
Values may be sent and summed in bfloat16 or wider, within the bound.
A program may use at most 64 MiB of HBM per device.

```python
import math
import jax
import jax.numpy as jnp
from jax import lax

D = 2560
HEAD_TOTAL = 80
HEAD_DIM = 64
STATE = 128
BLOCK = 256
TOK_DEV = 1024
TOKEN_TOTAL = 8192
INNER = 5120


def draw_log_decay(key, part):
    sequence_lanes = jax.random.split(key, 6)
    slow_share = 0.5
    chooser = jax.random.uniform(sequence_lanes[0], (HEAD_TOTAL,))
    fast_rate = jnp.exp(jax.random.uniform(sequence_lanes[1], (HEAD_TOTAL,), minval=jnp.log(1.0 / 60.0), maxval=jnp.log(1.0 / 25.0)))
    slow_rate = jnp.exp(jax.random.uniform(sequence_lanes[2], (HEAD_TOTAL,), minval=jnp.log(0.03), maxval=jnp.log(0.2))) / TOKEN_TOTAL
    head_decay_rates = jnp.where(chooser < slow_share, slow_rate, fast_rate)
    device_count = TOKEN_TOTAL // TOK_DEV
    shard_multiplier = jnp.exp(jax.random.uniform(sequence_lanes[3], (device_count, 1), minval=0.0, maxval=jnp.log(3.0)))
    shard_multiplier = jnp.repeat(shard_multiplier, TOK_DEV, axis=0)
    jaggedness = jnp.exp(jax.random.uniform(sequence_lanes[4], (TOKEN_TOTAL, HEAD_TOTAL), minval=jnp.log(0.5), maxval=jnp.log(2.0)))
    spike_locations = jax.random.randint(sequence_lanes[5], (2,), 0, TOKEN_TOTAL)
    spike_retain = jax.random.uniform(jax.random.fold_in(key, 7), (2, HEAD_TOTAL), minval=0.5, maxval=0.8)
    token_offsets = jnp.arange(TOKEN_TOTAL)[:, None]
    spike_events = jnp.where(token_offsets == spike_locations[0], jnp.log(spike_retain[0])[None, :], 0.0)
    spike_events = spike_events + jnp.where(token_offsets == spike_locations[1], jnp.log(spike_retain[1])[None, :], 0.0)
    return (-(head_decay_rates[None, :] * shard_multiplier * jaggedness) + spike_events).astype(jnp.float32)


def shard_levels(rng, extent, shards, least, largest):
    gain = 1.0
    for dim, shards_of in shards:
        draws = jax.random.uniform(jax.random.fold_in(jax.random.fold_in(rng, 6), dim), (shards_of,), jnp.float32, least / len(shards), largest / len(shards))
        gain = gain * jnp.repeat(jnp.exp(draws), extent[dim] // shards_of).reshape((-1,) + (1,) * (len(extent) - 1 - dim))
    return gain


def centred(own_key, dims, deviation, reach, pieces=(), dtype=jnp.bfloat16):
    loudness = shard_levels(own_key, dims, pieces, -0.22, 0.18) if pieces else 1.0
    drawn = jax.random.normal(own_key, dims, jnp.float32) * deviation * loudness
    return jnp.minimum(jnp.maximum(drawn, -reach), reach).astype(dtype)


def setup_inputs(seed: int = 0) -> dict:
    arg_keys = jax.random.split(jax.random.key(seed), 10)
    ssm_input = centred(arg_keys[0], (TOKEN_TOTAL, INNER), 1.0, 6.0, ((0, 8), (1, 4)))
    gate_input = centred(arg_keys[1], (TOKEN_TOTAL, INNER), 1.0, 6.0, ((0, 8), (1, 4)))
    state_in = centred(arg_keys[2], (TOKEN_TOTAL, STATE), 1.0, 6.0, ((0, 8),))
    state_out = centred(arg_keys[3], (TOKEN_TOTAL, STATE), STATE ** -0.5, 0.5, ((0, 8),))
    step_size = jnp.clip(jnp.exp(math.log(0.2) - 1.3862944 * jax.random.uniform(arg_keys[4], (TOKEN_TOTAL, HEAD_TOTAL), jnp.float32) ** shard_levels(arg_keys[4], (TOKEN_TOTAL, HEAD_TOTAL), ((0, 8), (1, 4)), -0.2, 0.2)), 0.05, 0.2)
    log_decay = draw_log_decay(jax.random.fold_in(arg_keys[9], 71), 0)
    skip_gain = jnp.clip(0.5 + 1.5 * jax.random.uniform(arg_keys[6], (HEAD_TOTAL,), jnp.float32) ** shard_levels(arg_keys[6], (HEAD_TOTAL,), ((0, 4),), -0.2, 0.2), 0.5, 2.0)
    norm_gain = jnp.clip(1.0 + 0.18 * jax.random.normal(arg_keys[7], (INNER,), jnp.float32), 0.099609375, 1.8984375).astype(jnp.bfloat16)
    out_weight = centred(arg_keys[8], (INNER, D), INNER ** -0.5, 0.078125, ((0, 4),))
    return dict(ssm_input=ssm_input, gate_input=gate_input, state_in=state_in, state_out=state_out, step_size=step_size, log_decay=log_decay, skip_gain=skip_gain, norm_gain=norm_gain, out_weight=out_weight)


def reference(ssm_input, gate_input, state_in, state_out, step_size, log_decay, skip_gain, norm_gain, out_weight):
    blocks = TOKEN_TOTAL // BLOCK
    inputs = ssm_input.reshape(blocks, BLOCK, HEAD_TOTAL, HEAD_DIM)
    gates = gate_input.reshape(blocks, BLOCK, INNER)
    writers = state_in.reshape(blocks, BLOCK, STATE)
    readers = state_out.reshape(blocks, BLOCK, STATE)
    steps_all = step_size.reshape(blocks, BLOCK, HEAD_TOTAL)
    decays_all = log_decay.reshape(blocks, BLOCK, HEAD_TOTAL)
    causal = jnp.arange(BLOCK)[:, None] >= jnp.arange(BLOCK)[None, :]
    gain_wide = norm_gain.astype(jnp.float32)

    def one_block(state, packed):
        inp, gate, writer, reader, steps, decay = packed
        level = jnp.cumsum(decay, axis=0)
        level_t = level.T
        intersection = jnp.dot(reader, writer.T, preferred_element_type=jnp.float32)
        gaps = level_t[:, :, None] - level_t[:, None, :]
        decays = jnp.where(causal[None], jnp.exp(jnp.where(causal[None], gaps, 0.0)), 0.0)
        score = (decays * intersection[None] * steps.T[:, None, :]).astype(jnp.bfloat16)
        within = jnp.einsum('hts,shp->thp', score.astype(jnp.float32), inp.astype(jnp.float32))
        from_carry = jnp.exp(level)[:, :, None] * jnp.einsum('tn,hpn->thp', reader.astype(jnp.float32), state, precision=lax.Precision.HIGHEST)
        closing = level[-1]
        weighted = ((jnp.exp(closing[None, :] - level) * steps)[:, :, None] * inp.astype(jnp.float32)).astype(jnp.bfloat16)
        own_state = jnp.einsum('shp,sn->hpn', weighted.astype(jnp.float32), writer.astype(jnp.float32))
        new_state = jnp.exp(closing)[:, None, None] * state + own_state
        mixed = within + from_carry + skip_gain[None, :, None] * inp.astype(jnp.float32)
        gated = mixed.reshape(BLOCK, INNER) * jax.nn.silu(gate.astype(jnp.float32))
        mean_sq = lax.optimization_barrier(jnp.mean(gated * gated, axis=1, keepdims=True))
        normed = (gated * lax.rsqrt(mean_sq + 1e-05) * gain_wide[None, :]).astype(jnp.bfloat16)
        result = jnp.dot(normed, out_weight, preferred_element_type=jnp.float32).astype(jnp.bfloat16)
        return (new_state, result)
    start = jnp.zeros((HEAD_TOTAL, HEAD_DIM, STATE), jnp.float32)
    final_state, results = lax.scan(one_block, start, (inputs, gates, writers, readers, steps_all, decays_all))
    return results.reshape(TOKEN_TOTAL, D)
```

```python
import functools

import jax
import jax.numpy as jnp
from jax import lax
from jax.experimental import pallas as pl
from jax.experimental.pallas import tpu as pltpu
from jax.sharding import PartitionSpec as P

BLOCK = 256
LOG2E = 1.4426950408889634
HI = lax.Precision.HIGHEST
F32 = jnp.float32
BF16 = jnp.bfloat16


def dotg(a, b, ca, cb, precision=None):
    return lax.dot_general(
        a, b, (((ca,), (cb,)), ((), ())), preferred_element_type=F32, precision=precision
    )


def kernel(
    cfg, x_ref, gate_hbm, b_ref, c_ref, stp_ref, ldt_ref, skip_ref, gain_ref, w_hbm,
    out_ref,
    gate, w, lev, lvs, levt, pref, lead, total, y, sg, u, ss,
    csend, crecv, psend, precv, xsend, xrecv, acc, ssrecv,
    load_sem, cs_sem, cr_sem, ps_sem, pr_sem, xs_sem, xr_sem, ss_sem, sr_sem,
):
    S, n, tok, ch, heads, D, cw, dc = cfg
    X, rd, blocks = n // 2, tok // n, tok // BLOCK
    hw = ch // heads
    per = 128 // hw
    pieces, nc = ch // 128, D // dc
    rows_chip = tok // X
    s, m = lax.axis_index("seq"), lax.axis_index("mp")
    chip, core = m // 2, lax.rem(m, 2)
    peer = chip * 2 + 1 - core

    load_gate = pltpu.make_async_copy(gate_hbm, gate, load_sem.at[0])
    load_w = pltpu.make_async_copy(w_hbm, w, load_sem.at[1])
    load_gate.start()
    load_w.start()

    barrier = pltpu.get_barrier_semaphore()
    for o in range(1, n):
        pl.semaphore_signal(barrier, inc=1, device_id={"mp": lax.rem(m + o, n)})
    for o in (1, S - 1):
        pl.semaphore_signal(barrier, inc=1, device_id={"seq": lax.rem(s + o, S)})
    pl.semaphore_wait(barrier, n + 1)

    spread = (
        lax.broadcasted_iota(jnp.int32, (heads, ch), 1) // hw
        == lax.broadcasted_iota(jnp.int32, (heads, ch), 0)
    )
    spread32, spread16 = spread.astype(F32), spread.astype(BF16)
    ti = lax.broadcasted_iota(jnp.int32, (BLOCK, BLOCK), 0)
    si = lax.broadcasted_iota(jnp.int32, (BLOCK, BLOCK), 1)
    tril = (ti >= si).astype(F32)
    triu = (ti <= si).astype(F32)
    eye = (ti == si).astype(F32)

    total[...] = jnp.zeros_like(total)
    ones = jnp.ones((8, ch), F32)

    def states(k, _):
        rows = pl.ds(pl.multiple_of(k * BLOCK, BLOCK), BLOCK)
        ldt = ldt_ref[:, rows] * LOG2E
        lst = jnp.log2(stp_ref[:, rows])
        level = dotg(tril, ldt, 1, 1, HI)
        shifted = level - dotg(eye, lst, 1, 1, HI)
        lev[rows, :] = level
        levt[k] = dotg(ldt, triu, 1, 0, HI) - lst
        closing = level[BLOCK - 1 : BLOCK, :]
        fac = jnp.exp2(closing - shifted).astype(BF16)
        decay = dotg(
            jnp.broadcast_to(jnp.exp2(closing), (8, heads)), spread32, 1, 0, HI
        )
        for j in range(ch // cw):
            cols = slice(j * cw, (j + 1) * cw)
            wide = dotg(fac, spread16[:, cols], 1, 0)
            weighted = (wide * x_ref[rows, cols].astype(F32)).astype(BF16)
            own = dotg(b_ref[rows, :], weighted, 0, 0)
            now = total[:, cols]
            pref[k, :, cols] = now
            total[:, cols] = decay[0:1, cols] * now + own
        before = jnp.where(k == 0, ones, lead[k])
        lead[k] = before
        lead[k + 1] = before * decay
        return 0

    lead[0] = ones
    lax.fori_loop(0, blocks, states, 0)

    def chain_copy(j):
        cols = pl.ds(pl.multiple_of(j * 128, 128), 128)
        return pltpu.make_async_remote_copy(
            src_ref=csend.at[j],
            dst_ref=crecv.at[j],
            send_sem=cs_sem.at[j],
            recv_sem=cr_sem.at[j],
            device_id={"seq": lax.rem(s + 1, S)},
        ), cols

    def chain(j, _):
        copy, cols = chain_copy(j)

        @pl.when(s == 0)
        def _():
            crecv[j] = jnp.zeros(crecv.shape[1:], BF16)

        @pl.when(s > 0)
        def _():
            copy.wait_recv()

        @pl.when(s < S - 1)
        def _():
            after = lead[blocks, 0:1, cols] * crecv[j].astype(F32) + total[:, cols]
            csend[j] = after.astype(BF16)
            copy.start()

        return 0

    load_gate.wait()
    lane = lax.broadcasted_iota(jnp.int32, (BLOCK, 128), 1)
    skip = dotg(jnp.broadcast_to(skip_ref[...], (8, heads)), spread32, 1, 0, HI)
    half = BLOCK // 2

    def within(k, _):
        @pl.when(k == (s * blocks) // S)
        def _():
            lax.fori_loop(0, pieces, chain, 0)

        rows = pl.ds(pl.multiple_of(k * BLOCK, BLOCK), BLOCK)
        inter = jnp.where(ti >= si, dotg(c_ref[rows, :], b_ref[rows, :], 1, 1), 0.0)
        top, low = inter[:half, :half], inter[half:, :]
        level = lev[rows, :]
        for q in range(pieces):
            cols = slice(q * 128, (q + 1) * 128)
            xp = x_ref[rows, cols]
            mix = skip[0:1, cols] * xp.astype(F32)
            res = None
            for p in range(per):
                h = q * per + p
                lt = level[:, h : h + 1]
                ls = levt[k, h : h + 1, :]
                g0 = jnp.exp2(jnp.minimum(lt[:half] - ls[:, :half], 0.0)) * top
                g1 = jnp.exp2(jnp.minimum(lt[half:] - ls, 0.0)) * low
                r = jnp.concatenate(
                    [dotg(g0.astype(BF16), xp[:half], 1, 0), dotg(g1.astype(BF16), xp, 1, 0)],
                    axis=0,
                )
                res = r if res is None else jnp.where(lane < p * hw, res, r)
            y[rows, cols] = mix + res
            v = gate[rows, cols].astype(F32)
            sg[rows, cols] = (v / (1.0 + jnp.exp(-v))).astype(BF16)
        return 0

    lax.fori_loop(0, blocks, within, 0)
    load_w.wait()

    def to_peer(i, j):
        return pltpu.make_async_remote_copy(
            src_ref=psend.at[i, j], dst_ref=precv.at[i, j],
            send_sem=ps_sem.at[i, j], recv_sem=pr_sem.at[i, j],
            device_id={"mp": peer},
        )

    def to_chip(i, j):
        return pltpu.make_async_remote_copy(
            src_ref=xsend.at[i, j], dst_ref=xrecv.at[i, j],
            send_sem=xs_sem.at[i, j], recv_sem=xr_sem.at[i, j],
            device_id={"mp": lax.rem(chip + 1 + i, X) * 2 + core},
        )

    def ss_copy(o):
        t = lax.rem(m + o, n)
        return pltpu.make_async_remote_copy(
            src_ref=ss.at[t], dst_ref=ssrecv.at[o],
            send_sem=ss_sem.at[o], recv_sem=sr_sem.at[o],
            device_id={"mp": t},
        )

    unit = jnp.ones((8, cw), BF16)
    gaincols = gain_ref[...].astype(F32)

    def gating(r0):
        k = r0 // BLOCK
        rows = pl.ds(pl.multiple_of(r0, BLOCK), BLOCK)
        grow = jnp.exp2(lev[rows, :]).astype(BF16)
        reader = c_ref[rows, :]
        sq = jnp.zeros((8, BLOCK), F32)
        for j in range(ch // cw):
            cols = slice(j * cw, (j + 1) * cw)
            came = jnp.concatenate(
                [crecv[j * cw // 128 + a] for a in range(cw // 128)], axis=1
            ).astype(F32)
            carried = (pref[k, :, cols] + lead[k, 0:1, cols] * came).astype(BF16)
            fc = dotg(reader, carried, 1, 0) * dotg(grow, spread16[:, cols], 1, 0)
            gated = sg[rows, cols].astype(F32) * (y[rows, cols] + fc)
            sq = sq + dotg(unit, (gated * gated).astype(BF16), 1, 1)
            u[rows, cols] = (gated * gaincols[:, cols]).astype(BF16)
        for a in range(BLOCK // rd):
            ss[r0 // rd + a] = sq[:, a * rd : (a + 1) * rd]

    for i in range(X):
        c = lax.rem(chip + 1 + i, X)
        base = c * rows_chip

        def gate_block(b, _):
            gating(base + b * BLOCK)
            return 0

        lax.fori_loop(0, rows_chip // BLOCK, gate_block, 0)
        if i == X - 1:

            def send_ss(o, _):
                ss_copy(o).start()
                return 0

            lax.fori_loop(1, n, send_ss, 0)
        theirs = pl.ds(pl.multiple_of(base + (1 - core) * rd, rd), rd)
        mine = pl.ds(pl.multiple_of(base + core * rd, rd), rd)

        def forward(j):
            to_peer(i, j).wait_recv()
            xsend[i, j] = (acc[j] + precv[i, j].astype(F32)).astype(BF16)
            to_chip(i, j).start()

        def project(j, _):
            cols = pl.ds(pl.multiple_of(j * dc, dc), dc)
            psend[i, j] = dotg(u[theirs, :], w[:, cols], 1, 0).astype(BF16)
            to_peer(i, j).start()
            if i < X - 1:
                @pl.when(j > 0)
                def _():
                    forward(j - 1)
            acc[j] = dotg(u[mine, :], w[:, cols], 1, 0)
            return 0

        lax.fori_loop(0, nc, project, 0)
        if i < X - 1:
            forward(nc - 1)

    sq = ss[m]
    for o in range(1, n):
        ss_copy(o).wait_recv()
        sq = sq + ssrecv[o]
    mean = dotg(sq, jnp.full((8, 128), 0.125, F32), 0, 0, HI) / (ch * n)
    scale = lax.rsqrt(mean + 1e-05)
    scale = jnp.concatenate([scale] * (dc // 128), axis=1)
    for j in range(nc):
        to_peer(X - 1, j).wait_recv()
        value = acc[j] + precv[X - 1, j].astype(F32)
        for i in range(X - 1):
            to_chip(i, j).wait_recv()
            value = value + xrecv[i, j].astype(F32)
        out_ref[:, j * dc : (j + 1) * dc] = (value * scale).astype(BF16)

    for j in range(nc):
        for i in range(X):
            to_peer(i, j).wait_send()
        for i in range(X - 1):
            to_chip(i, j).wait_send()
    for o in range(1, n):
        ss_copy(o).wait_send()

    @pl.when(s < S - 1)
    def _():
        for j in range(pieces):
            chain_copy(j)[0].wait_send()


def body(S, n, x, gate, b, c, step, log_decay, skip, gain, w):
    tok, ch = x.shape
    heads, st, D = step.shape[1], b.shape[1], w.shape[1]
    X, rd, blocks = n // 2, tok // n, tok // BLOCK
    cw = 256 if ch % 256 == 0 else 128
    dc = 512 if D % 512 == 0 else 128
    pieces, nc = ch // 128, D // dc
    cfg = (S, n, tok, ch, heads, D, cw, dc)
    vmem = pl.BlockSpec(memory_space=pltpu.VMEM)
    hbm = pl.BlockSpec(memory_space=pl.ANY)
    V, DMA = pltpu.VMEM, pltpu.SemaphoreType.DMA
    return pl.pallas_call(
        functools.partial(kernel, cfg),
        out_shape=jax.ShapeDtypeStruct((rd, D), BF16),
        in_specs=[vmem, hbm, vmem, vmem, vmem, vmem, vmem, vmem, hbm],
        out_specs=vmem,
        scratch_shapes=[
            V((tok, ch), BF16),
            V(w.shape, BF16),
            V((tok, heads), F32),
            V((8, 128), F32),
            V((blocks, heads, BLOCK), F32),
            V((blocks, st, ch), F32),
            V((blocks + 1, 8, ch), F32),
            V((st, ch), F32),
            V((tok, ch), F32),
            V((tok, ch), BF16),
            V((tok, ch), BF16),
            V((n, 8, rd), F32),
            V((pieces, st, 128), BF16),
            V((pieces, st, 128), BF16),
            V((X, nc, rd, dc), BF16),
            V((X, nc, rd, dc), BF16),
            V((max(X - 1, 1), nc, rd, dc), BF16),
            V((max(X - 1, 1), nc, rd, dc), BF16),
            V((nc, rd, dc), F32),
            V((n, 8, rd), F32),
            DMA((2,)),
            DMA((pieces,)),
            DMA((pieces,)),
            DMA((X, nc)),
            DMA((X, nc)),
            DMA((max(X - 1, 1), nc)),
            DMA((max(X - 1, 1), nc)),
            DMA((n,)),
            DMA((n,)),
        ],
        compiler_params=pltpu.CompilerParams(
            collective_id=0, has_side_effects=True, vmem_limit_bytes=60 * 1024 * 1024
        ),
    )(x, gate, b, c, step.T, log_decay.T, skip[None, :], gain[None, :], w)


def solution(mesh):
    placed = (
        P("seq", "mp"),
        P("seq", "mp"),
        P("seq", None),
        P("seq", None),
        P("seq", "mp"),
        P("seq", "mp"),
        P("mp"),
        P("mp"),
        P("mp", None),
    )
    return jax.shard_map(
        functools.partial(body, mesh.shape["seq"], mesh.shape["mp"]),
        mesh=mesh, in_specs=placed, out_specs=P(("seq", "mp"), None), check_vma=False,
    )
```

```python
import functools

import jax
import jax.numpy as jnp
from jax import lax
from jax.experimental import pallas as pl
from jax.experimental.pallas import tpu as pltpu
from jax.sharding import PartitionSpec as P

BLOCK = 256
LOG2E = 1.4426950408889634
HI = lax.Precision.HIGHEST
F32 = jnp.float32
BF16 = jnp.bfloat16


def dotg(a, b, ca, cb, precision=None):
    return lax.dot_general(
        a, b, (((ca,), (cb,)), ((), ())), preferred_element_type=F32, precision=precision
    )


def kernel(
    cfg, x_ref, gate_hbm, b_ref, c_ref, stp_ref, ldt_ref, skip_ref, gain_ref, w_hbm,
    out_ref,
    gate, w, lev, lvs, levt, pref, lead, total, y, sg, u, ss,
    dpart, gsend, grecv, fsend, prefix, csend, crecv, psend, precv, xsend, xrecv, acc, ssrecv,
    load_sem, d_sem, gs_sem, gr_sem, fs_sem, fr_sem, cs_sem, cr_sem, ps_sem, pr_sem, xs_sem, xr_sem, ss_sem, sr_sem,
):
    S, n, tok, ch, heads, D, cw, dc = cfg
    X, rd, blocks = n // 2, tok // n, tok // BLOCK
    hw = ch // heads
    per = 128 // hw
    pieces, nc = ch // 128, D // dc
    rows_chip = tok // X
    s, m = lax.axis_index("seq"), lax.axis_index("mp")
    chip, core = m // 2, lax.rem(m, 2)
    peer = chip * 2 + 1 - core
    odd = lax.rem(s, 2)
    mate = s + 1 - 2 * odd

    load_gate = pltpu.make_async_copy(gate_hbm, gate, load_sem.at[0])
    load_w = pltpu.make_async_copy(w_hbm, w, load_sem.at[1])
    load_gate.start()
    load_w.start()

    barrier = pltpu.get_barrier_semaphore()
    for o in range(1, n):
        pl.semaphore_signal(barrier, inc=1, device_id={"mp": lax.rem(m + o, n)})
    for o in (2, S - 2):
        pl.semaphore_signal(barrier, inc=1, device_id={"seq": lax.rem(s + o, S)})
    pl.semaphore_signal(barrier, inc=1, device_id={"seq": mate})
    pl.semaphore_wait(barrier, n + 2)

    spread = (
        lax.broadcasted_iota(jnp.int32, (heads, ch), 1) // hw
        == lax.broadcasted_iota(jnp.int32, (heads, ch), 0)
    )
    spread32, spread16 = spread.astype(F32), spread.astype(BF16)
    ti = lax.broadcasted_iota(jnp.int32, (BLOCK, BLOCK), 0)
    si = lax.broadcasted_iota(jnp.int32, (BLOCK, BLOCK), 1)
    tril = (ti >= si).astype(F32)
    triu = (ti <= si).astype(F32)
    eye = (ti == si).astype(F32)

    total[...] = jnp.zeros_like(total)
    ones = jnp.ones((8, ch), F32)

    def states(k, _):
        rows = pl.ds(pl.multiple_of(k * BLOCK, BLOCK), BLOCK)
        ldt = ldt_ref[:, rows] * LOG2E
        lst = jnp.log2(stp_ref[:, rows])
        level = dotg(tril, ldt, 1, 1, HI)
        shifted = level - dotg(eye, lst, 1, 1, HI)
        lev[rows, :] = level
        levt[k] = dotg(ldt, triu, 1, 0, HI) - lst
        closing = level[BLOCK - 1 : BLOCK, :]
        fac = jnp.exp2(closing - shifted).astype(BF16)
        decay = dotg(
            jnp.broadcast_to(jnp.exp2(closing), (8, heads)), spread32, 1, 0, HI
        )
        for j in range(ch // cw):
            cols = slice(j * cw, (j + 1) * cw)
            wide = dotg(fac, spread16[:, cols], 1, 0)
            weighted = (wide * x_ref[rows, cols].astype(F32)).astype(BF16)
            own = dotg(b_ref[rows, :], weighted, 0, 0)
            now = total[:, cols]
            pref[k, :, cols] = now
            total[:, cols] = decay[0:1, cols] * now + own
        before = jnp.where(k == 0, ones, lead[k])
        lead[k] = before
        lead[k + 1] = before * decay
        return 0

    lead[0] = ones
    lax.fori_loop(0, blocks, states, 0)

    n0 = pieces - pieces // 2
    off, count = odd * n0, jnp.where(odd == 0, n0, pieces - n0)
    away, left = (1 - odd) * n0, pieces - count

    def remote(src, dst, send, recv, device):
        return pltpu.make_async_remote_copy(
            src_ref=src, dst_ref=dst, send_sem=send, recv_sem=recv, device_id={"seq": device}
        )

    decay_copy = remote(lead.at[blocks], dpart, d_sem.at[0], d_sem.at[1], mate)

    def give(j):
        return remote(gsend.at[j], grecv.at[j], gs_sem.at[j], gr_sem.at[j], mate)

    def hand(j):
        return remote(csend.at[j], crecv.at[j], cs_sem.at[j], cr_sem.at[j], lax.rem(s + 2, S))

    def back(j):
        return remote(fsend.at[j], prefix.at[j], fs_sem.at[j], fr_sem.at[j], mate)

    def lanes(j):
        return pl.ds(pl.multiple_of(j * 128, 128), 128)

    decay_copy.start()

    def give_piece(a, _):
        j = away + a
        gsend[j] = total[:, lanes(j)].astype(BF16)
        give(j).start()
        return 0

    lax.fori_loop(0, left, give_piece, 0)

    def chain(a):
        j = off + a
        cols = lanes(j)

        @pl.when(a == 0)
        def _():
            decay_copy.wait_recv()

        give(j).wait_recv()

        @pl.when(s < 2)
        def _():
            crecv[j] = jnp.zeros(crecv.shape[1:], BF16)

        @pl.when(s >= 2)
        def _():
            hand(j).wait_recv()

        even = odd == 0
        own, other = total[:, cols], grecv[j].astype(F32)
        d_own, d_other = lead[blocks, 0:1, cols], dpart[0:1, cols]
        before = crecv[j].astype(F32)
        middle = jnp.where(even, d_own, d_other) * before + jnp.where(even, own, other)

        @pl.when(s < S - 2)
        def _():
            after = jnp.where(even, d_other, d_own) * middle + jnp.where(even, other, own)
            csend[j] = after.astype(BF16)
            hand(j).start()

        fsend[j] = jnp.where(even, middle, before).astype(BF16)
        back(j).start()
        prefix[j] = jnp.where(even, before, middle).astype(BF16)

    load_gate.wait()
    lane = lax.broadcasted_iota(jnp.int32, (BLOCK, 128), 1)
    skip = dotg(jnp.broadcast_to(skip_ref[...], (8, heads)), spread32, 1, 0, HI)
    half = BLOCK // 2
    units = blocks * pieces
    first = units // 4 + (s // 2) * (units - units // 4 - 2 * n0) // max(S // 2 - 1, 1)

    def within(k, _):
        rows = pl.ds(pl.multiple_of(k * BLOCK, BLOCK), BLOCK)
        inter = jnp.where(ti >= si, dotg(c_ref[rows, :], b_ref[rows, :], 1, 1), 0.0)
        inter = inter.astype(BF16)
        top, low = inter[:half, :half], inter[half:, :]
        level = lev[rows, :]
        grow = jnp.exp2(level).astype(BF16)
        for q in range(pieces):
            cols = slice(q * 128, (q + 1) * 128)
            xp = x_ref[rows, cols]
            mix = skip[0:1, cols] * xp.astype(F32)
            res = None
            for p in range(per):
                h = q * per + p
                lt = level[:, h : h + 1]
                ls = levt[k, h : h + 1, :]
                g0 = jnp.exp2(jnp.minimum(lt[:half] - ls[:, :half], 0.0).astype(BF16)) * top
                g1 = jnp.exp2(jnp.minimum(lt[half:] - ls, 0.0).astype(BF16)) * low
                r = jnp.concatenate(
                    [dotg(g0, xp[:half], 1, 0), dotg(g1, xp, 1, 0)],
                    axis=0,
                )
                res = r if res is None else jnp.where(lane < p * hw, res, r)
            v = gate[rows, cols].astype(F32)
            silu = v / (1.0 + jnp.exp(-v))
            y[rows, cols] = (mix + res) * silu
            sg[rows, cols] = (silu * dotg(grow, spread16[:, cols], 1, 0)).astype(BF16)
            turn = k * pieces + q - first

            @pl.when((turn >= 0) & (turn < 2 * count) & (lax.rem(turn + units, 2) == 0))
            def _():
                chain(turn // 2)

        return 0

    lax.fori_loop(0, blocks, within, 0)
    load_w.wait()

    def settle(a, _):
        back(away + a).wait_recv()
        return 0

    lax.fori_loop(0, left, settle, 0)

    def to_peer(i, j):
        return pltpu.make_async_remote_copy(
            src_ref=psend.at[i, j], dst_ref=precv.at[i, j],
            send_sem=ps_sem.at[i, j], recv_sem=pr_sem.at[i, j],
            device_id={"mp": peer},
        )

    def to_chip(i, j):
        return pltpu.make_async_remote_copy(
            src_ref=xsend.at[i, j], dst_ref=xrecv.at[i, j],
            send_sem=xs_sem.at[i, j], recv_sem=xr_sem.at[i, j],
            device_id={"mp": lax.rem(chip + 1 + i, X) * 2 + core},
        )

    def ss_copy(o):
        t = lax.rem(m + o, n)
        return pltpu.make_async_remote_copy(
            src_ref=ss.at[t], dst_ref=ssrecv.at[o],
            send_sem=ss_sem.at[o], recv_sem=sr_sem.at[o],
            device_id={"mp": t},
        )

    unit = jnp.ones((8, cw), BF16)
    gaincols = gain_ref[...].astype(F32)

    def gating(r0):
        k = r0 // BLOCK
        rows = pl.ds(pl.multiple_of(r0, BLOCK), BLOCK)
        reader = c_ref[rows, :]
        sq = jnp.zeros((8, BLOCK), F32)
        for j in range(ch // cw):
            cols = slice(j * cw, (j + 1) * cw)
            came = jnp.concatenate(
                [prefix[j * cw // 128 + a] for a in range(cw // 128)], axis=1
            ).astype(F32)
            carried = (pref[k, :, cols] + lead[k, 0:1, cols] * came).astype(BF16)
            gated = y[rows, cols] + sg[rows, cols].astype(F32) * dotg(reader, carried, 1, 0)
            sq = sq + dotg(unit, (gated * gated).astype(BF16), 1, 1)
            u[rows, cols] = (gated * gaincols[:, cols]).astype(BF16)
        for a in range(BLOCK // rd):
            ss[r0 // rd + a] = sq[:, a * rd : (a + 1) * rd]

    for i in range(X):
        c = lax.rem(chip + 1 + i, X)
        base = c * rows_chip

        def gate_block(b, _):
            gating(base + b * BLOCK)
            return 0

        lax.fori_loop(0, rows_chip // BLOCK, gate_block, 0)
        if i == X - 1:

            def send_ss(o, _):
                ss_copy(o).start()
                return 0

            lax.fori_loop(1, n, send_ss, 0)
        theirs = pl.ds(pl.multiple_of(base + (1 - core) * rd, rd), rd)
        mine = pl.ds(pl.multiple_of(base + core * rd, rd), rd)

        def forward(j):
            to_peer(i, j).wait_recv()
            xsend[i, j] = (acc[j] + precv[i, j].astype(F32)).astype(BF16)
            to_chip(i, j).start()

        def project(j, _):
            cols = pl.ds(pl.multiple_of(j * dc, dc), dc)
            psend[i, j] = dotg(u[theirs, :], w[:, cols], 1, 0).astype(BF16)
            to_peer(i, j).start()
            if i < X - 1:
                @pl.when(j > 0)
                def _():
                    forward(j - 1)
            acc[j] = dotg(u[mine, :], w[:, cols], 1, 0)
            return 0

        lax.fori_loop(0, nc, project, 0)
        if i < X - 1:
            forward(nc - 1)

    sq = ss[m]
    for o in range(1, n):
        ss_copy(o).wait_recv()
        sq = sq + ssrecv[o]
    mean = dotg(sq, jnp.full((8, 128), 0.125, F32), 0, 0, HI) / (ch * n)
    scale = lax.rsqrt(mean + 1e-05)
    scale = jnp.concatenate([scale] * (dc // 128), axis=1)
    for j in range(nc):
        to_peer(X - 1, j).wait_recv()
        value = acc[j] + precv[X - 1, j].astype(F32)
        for i in range(X - 1):
            to_chip(i, j).wait_recv()
            value = value + xrecv[i, j].astype(F32)
        out_ref[:, j * dc : (j + 1) * dc] = (value * scale).astype(BF16)

    for j in range(nc):
        for i in range(X):
            to_peer(i, j).wait_send()
        for i in range(X - 1):
            to_chip(i, j).wait_send()
    for o in range(1, n):
        ss_copy(o).wait_send()

    decay_copy.wait_send()

    def drain_give(a, _):
        give(away + a).wait_send()
        return 0

    lax.fori_loop(0, left, drain_give, 0)

    def drain(a, _):
        back(off + a).wait_send()

        @pl.when(s < S - 2)
        def _():
            hand(off + a).wait_send()

        return 0

    lax.fori_loop(0, count, drain, 0)


def body(S, n, x, gate, b, c, step, log_decay, skip, gain, w):
    tok, ch = x.shape
    heads, st, D = step.shape[1], b.shape[1], w.shape[1]
    X, rd, blocks = n // 2, tok // n, tok // BLOCK
    cw = 256 if ch % 256 == 0 else 128
    dc = 512 if D % 512 == 0 else 128
    pieces, nc = ch // 128, D // dc
    cfg = (S, n, tok, ch, heads, D, cw, dc)
    vmem = pl.BlockSpec(memory_space=pltpu.VMEM)
    hbm = pl.BlockSpec(memory_space=pl.ANY)
    V, DMA = pltpu.VMEM, pltpu.SemaphoreType.DMA
    return pl.pallas_call(
        functools.partial(kernel, cfg),
        out_shape=jax.ShapeDtypeStruct((rd, D), BF16),
        in_specs=[vmem, hbm, vmem, vmem, vmem, vmem, vmem, vmem, hbm],
        out_specs=vmem,
        scratch_shapes=[
            V((tok, ch), BF16),
            V(w.shape, BF16),
            V((tok, heads), F32),
            V((8, 128), F32),
            V((blocks, heads, BLOCK), F32),
            V((blocks, st, ch), F32),
            V((blocks + 1, 8, ch), F32),
            V((st, ch), F32),
            V((tok, ch), F32),
            V((tok, ch), BF16),
            V((tok, ch), BF16),
            V((n, 8, rd), F32),
            V((8, ch), F32),
            V((pieces, st, 128), BF16),
            V((pieces, st, 128), BF16),
            V((pieces, st, 128), BF16),
            V((pieces, st, 128), BF16),
            V((pieces, st, 128), BF16),
            V((pieces, st, 128), BF16),
            V((X, nc, rd, dc), BF16),
            V((X, nc, rd, dc), BF16),
            V((max(X - 1, 1), nc, rd, dc), BF16),
            V((max(X - 1, 1), nc, rd, dc), BF16),
            V((nc, rd, dc), F32),
            V((n, 8, rd), F32),
            DMA((2,)),
            DMA((2,)),
            DMA((pieces,)),
            DMA((pieces,)),
            DMA((pieces,)),
            DMA((pieces,)),
            DMA((pieces,)),
            DMA((pieces,)),
            DMA((X, nc)),
            DMA((X, nc)),
            DMA((max(X - 1, 1), nc)),
            DMA((max(X - 1, 1), nc)),
            DMA((n,)),
            DMA((n,)),
        ],
        compiler_params=pltpu.CompilerParams(
            collective_id=0, has_side_effects=True, vmem_limit_bytes=60 * 1024 * 1024
        ),
    )(x, gate, b, c, step.T, log_decay.T, skip[None, :], gain[None, :], w)


def solution(mesh):
    placed = (
        P("seq", "mp"),
        P("seq", "mp"),
        P("seq", None),
        P("seq", None),
        P("seq", "mp"),
        P("seq", "mp"),
        P("mp"),
        P("mp"),
        P("mp", None),
    )
    return jax.shard_map(
        functools.partial(body, mesh.shape["seq"], mesh.shape["mp"]),
        mesh=mesh, in_specs=placed, out_specs=P(("seq", "mp"), None), check_vma=False,
    )
```
